128 devices in a mesh: blk: 8 (over z, x_lo), head: 16 (over y, x_hi, core).
Axes of the slice: x: 4 (x_hi: 2, x_lo: 2; x = x_hi * 2 + x_lo), y: 4, z: 4, core: 2. Of those that a mesh axis runs over, the one named last changes fastest.
Arguments:
- latent: float32 [128, 512, 256], P('blk', 'head'), may hold values from -6 to 6
- local_gain: float32 [256], replicated, may hold values from 0.5 to 1.5
- local_project: float32 [256, 768], replicated, may hold values from -0.375 to 0.375
- local_output: float32 [256, 256], replicated, may hold values from -0.375 to 0.375
- local_scale: float32 [4], replicated, may hold values from 2 to 500
- merge_first: float32 [1024, 384], replicated, may hold values from -0.1875 to 0.1875
- merge_second: float32 [1536, 512], replicated, may hold values from -0.15625 to 0.15625
- global_gain: float32 [512], replicated, may hold values from 0.5 to 1.5
- global_project: float32 [512, 1536], replicated, may hold values from -0.25 to 0.25
- global_output: float32 [512, 512], replicated, may hold values from -0.25 to 0.25
- global_scale: float32 [8], replicated, may hold values from 2 to 500
- split_second: float32 [512, 1536], replicated, may hold values from -0.25 to 0.25
- split_first: float32 [384, 1024], replicated, may hold values from -0.3125 to 0.3125
Outputs:
- refined: float32 [128, 512, 256], P('blk', 'head')
The draws below stay inside these ranges and needn't reach their ends.
All inputs are finite; a program needn't handle non-finite values.
Results may differ from the reference program's by a relative error of at most 0.0003.
Values sent between devices are 32-bit elements; how exact they have to be, the bound alone decides.
No kernel may reach another device: no remote copies, remote signals or barrier semaphores. Data moves between devices by JAX's collectives and lax.ppermute only.
A program may use at most 128 MiB of HBM per device.

```python
import math
import jax
import jax.numpy as jnp
from jax import lax

C0 = 256
HEAD0 = 64
CM = 384
CG = 512
HEADS_G = 8
HEAD_G = 64
HEIGHT = 128
BREADTH = 512


def scale_draw(key, how_many):
    lower, upper = (2.0, 20.0)
    exponent = jax.random.uniform(key, (how_many,), jnp.float32, math.log(lower), math.log(upper))
    return jnp.exp(exponent)


def draw_local_scale(key, part):
    return scale_draw(jax.random.fold_in(key, 11), C0 // HEAD0)


def draw_global_scale(key, part):
    return scale_draw(jax.random.fold_in(key, 23), HEADS_G)


def block_levels(rng, dims, pieces, smallest, top_value):
    def one(dim, blocks):
        steps = jax.random.uniform(jax.random.fold_in(jax.random.fold_in(rng, 6), dim), (blocks,), jnp.float32, smallest / len(pieces), top_value / len(pieces))
        return jnp.repeat(jnp.exp(steps), dims[dim] // blocks).reshape((-1,) + (1,) * (len(dims) - dim - 1))

    level = one(*pieces[0])
    for cut in pieces[1:]:
        level = level * one(*cut)
    return level


def normal_values(own_key, extent, scale, bound, shards=(), held_as=jnp.bfloat16):
    array = scale * jax.random.normal(own_key, extent, jnp.float32)
    if shards:
        array = array * block_levels(own_key, extent, shards, -0.22, 0.18)
    return jnp.clip(array, -bound, bound).astype(held_as)


def setup_inputs(seed: int = 0) -> dict:
    key_list = jax.random.split(jax.random.key(seed), 14)
    return {
        "latent": normal_values(key_list[0], (HEIGHT, BREADTH, C0), 1.0, 6.0, ((0, 8), (1, 16)), jnp.float32),
        "local_gain": jnp.clip(1.0 + 0.1 * jax.random.normal(key_list[1], (C0,), jnp.float32), 0.5, 1.5),
        "local_project": normal_values(key_list[2], (C0, 3 * C0), C0 ** -0.5, 0.375, (), jnp.float32),
        "local_output": normal_values(key_list[3], (C0, C0), C0 ** -0.5, 0.375, (), jnp.float32),
        "local_scale": draw_local_scale(jax.random.fold_in(key_list[13], 71), 0),
        "merge_first": normal_values(key_list[5], (4 * C0, CM), (4 * C0) ** -0.5, 0.1875, (), jnp.float32),
        "merge_second": normal_values(key_list[6], (4 * CM, CG), (4 * CM) ** -0.5, 0.15625, (), jnp.float32),
        "global_gain": jnp.clip(1.0 + 0.1 * jax.random.normal(key_list[7], (CG,), jnp.float32), 0.5, 1.5),
        "global_project": normal_values(key_list[8], (CG, 3 * CG), CG ** -0.5, 0.25, (), jnp.float32),
        "global_output": normal_values(key_list[9], (CG, CG), CG ** -0.5, 0.25, (), jnp.float32),
        "global_scale": draw_global_scale(jax.random.fold_in(key_list[13], 71), 0),
        "split_second": normal_values(key_list[11], (CG, 4 * CM), CG ** -0.5, 0.25, (), jnp.float32),
        "split_first": normal_values(key_list[12], (CM, 4 * C0), CM ** -0.5, 0.3125, (), jnp.float32),
    }


EPSILON = 1e-06
FLOOR_VALUE = 0.5
PRECISE = lax.Precision.HIGHEST

def matmul(left, right):
    return jnp.dot(left, right, precision=PRECISE, preferred_element_type=jnp.float32)

def rms_scale(values, gains):
    return values * lax.rsqrt(lax.optimization_barrier(jnp.mean(values * values, axis=-1, keepdims=True)) + EPSILON) * gains

def unit_rows(values):
    return values * lax.rsqrt(lax.optimization_barrier(jnp.mean(values * values, axis=-1, keepdims=True)) + EPSILON)

def floor_rows(values):
    return values * lax.rsqrt(jnp.maximum(lax.optimization_barrier(jnp.mean(values * values, axis=-1, keepdims=True)), FLOOR_VALUE))

def window_attention(queries, keys_pad, values_pad, valid, scales):
    query_rows, query_cols, head_width = (queries.shape[0], queries.shape[1], queries.shape[3])
    factor = scales / head_width
    scores = []
    for offset_row in range(7):
        for offset_col in range(7):
            nearby = keys_pad[offset_row:offset_row + query_rows, offset_col:offset_col + query_cols]
            one_score = lax.optimization_barrier(jnp.sum(queries * nearby, axis=-1)) * factor
            inside = valid[offset_row:offset_row + query_rows, offset_col:offset_col + query_cols, None] > 0
            scores.append(jnp.where(inside, one_score, -jnp.inf))
    stacked = jnp.stack(scores)
    maximum = lax.optimization_barrier(jnp.max(stacked, axis=0))
    weights = jnp.exp(stacked - maximum)
    weight_sum = lax.optimization_barrier(jnp.sum(weights, axis=0))
    mixture = jnp.zeros_like(queries)
    position = 0
    for offset_row in range(7):
        for offset_col in range(7):
            nearby = values_pad[offset_row:offset_row + query_rows, offset_col:offset_col + query_cols]
            mixture = mixture + weights[position][..., None] * nearby
            position = position + 1
    return mixture / weight_sum[..., None]

def merge_cells(grid_in):
    grid_rows, grid_cols, channels = grid_in.shape
    moved = grid_in.reshape(grid_rows // 2, 2, grid_cols // 2, 2, channels).transpose(0, 2, 1, 3, 4)
    return moved.reshape(grid_rows // 2, grid_cols // 2, 4 * channels)

def split_cells(grid_in, channels):
    grid_rows, grid_cols = (grid_in.shape[0], grid_in.shape[1])
    moved = grid_in.reshape(grid_rows, grid_cols, 2, 2, channels).transpose(0, 2, 1, 3, 4)
    return moved.reshape(2 * grid_rows, 2 * grid_cols, channels)

def global_attention(global_queries, global_keys, global_values, scales):
    token_count = global_queries.shape[0]
    block_rows = math.gcd(token_count, 1024)

    def one_head(head_items):
        head_queries, head_keys, head_values, head_scale = head_items
        factor = head_scale / head_queries.shape[1]

        def one_block(block_queries):
            scores = matmul(block_queries, head_keys.T) * factor
            maximum = lax.optimization_barrier(jnp.max(scores, axis=1, keepdims=True))
            weights = jnp.exp(scores - maximum)
            return matmul(weights, head_values) / lax.optimization_barrier(jnp.sum(weights, axis=1, keepdims=True))
        blocked = head_queries.reshape(token_count // block_rows, block_rows, head_queries.shape[1])
        return lax.map(one_block, blocked).reshape(token_count, head_queries.shape[1])
    outputs = lax.map(one_head, (jnp.transpose(global_queries, (1, 0, 2)), jnp.transpose(global_keys, (1, 0, 2)), jnp.transpose(global_values, (1, 0, 2)), scales))
    return jnp.transpose(outputs, (1, 0, 2))

def reference(latent, local_gain, local_project, local_output, local_scale, merge_first, merge_second, global_gain, global_project, global_output, global_scale, split_second, split_first):
    height, breadth = (latent.shape[0], latent.shape[1])
    heads_zero = C0 // HEAD0
    normed = rms_scale(latent, local_gain)
    projected = matmul(normed.reshape(-1, C0), local_project).reshape(height, breadth, 3, heads_zero, HEAD0)
    local_queries = unit_rows(projected[:, :, 0])
    local_keys = unit_rows(projected[:, :, 1])
    local_values = projected[:, :, 2]
    padding = ((3, 3), (3, 3), (0, 0), (0, 0))
    valid = jnp.pad(jnp.ones((height, breadth), jnp.float32), 3)
    attended = window_attention(local_queries, jnp.pad(local_keys, padding), jnp.pad(local_values, padding), valid, local_scale)
    level_zero = latent + matmul(attended.reshape(-1, C0), local_output).reshape(height, breadth, C0)
    level_one = matmul(merge_cells(level_zero).reshape(-1, 4 * C0), merge_first).reshape(height // 2, breadth // 2, CM)
    level_two = matmul(merge_cells(level_one).reshape(-1, 4 * CM), merge_second)
    normed_two = rms_scale(level_two, global_gain)
    global_proj = matmul(normed_two, global_project).reshape(-1, HEADS_G, 3, HEAD_G)
    global_queries = floor_rows(global_proj[:, :, 0])
    global_keys = floor_rows(global_proj[:, :, 1])
    global_values = global_proj[:, :, 2]
    attention_out = global_attention(global_queries, global_keys, global_values, global_scale)
    global_mixed = level_two + matmul(attention_out.reshape(-1, CG), global_output)
    up_one = split_cells(matmul(global_mixed, split_second).reshape(height // 4, breadth // 4, 4 * CM), CM) + level_one
    refined = split_cells(matmul(up_one.reshape(-1, CM), split_first).reshape(height // 2, breadth // 2, 4 * C0), C0) + level_zero
    return refined
```

```python
import jax
import jax.numpy as jnp
from jax import lax
from jax.experimental import pallas as pl
from jax.experimental.pallas import tpu as pltpu
from jax.sharding import Mesh, PartitionSpec as P

C0 = 256
CM = 384
CG = 512
HEADS0 = 4
HEADS_G = 8
HEAD = 64
ROWS = 16
COLS = 32
PAD_ROWS = ROWS + 6
PAD_COLS = 40
BLOCK = 4
KEYS = (BLOCK + 6) * PAD_COLS
EPSILON = 1e-06
FLOOR_VALUE = 0.5
NEG = -1e30
HIGH = lax.Precision.HIGH
ZX = ("z", "xh", "xl")
YC = ("y", "c")
CLASSES = [(a1, b1, a2, b2) for a1 in (0, 1) for b1 in (0, 1) for a2 in (0, 1) for b2 in (0, 1)]


def mm(a, b):
    return jnp.dot(a, b, precision=HIGH, preferred_element_type=jnp.float32)


def mm_t(a, b):
    return lax.dot_general(
        a, b, (((1,), (1,)), ((), ())), precision=HIGH, preferred_element_type=jnp.float32
    )


def iota(shape, dim):
    return lax.broadcasted_iota(jnp.int32, shape, dim)


def head_mean(x):
    n = x.shape[1]
    same = iota((n, n), 0) // HEAD == iota((n, n), 1) // HEAD
    return mm(x * x, jnp.where(same, 1.0 / HEAD, 0.0))


def rms(x, gain):
    return x * lax.rsqrt(jnp.mean(x * x, axis=-1, keepdims=True) + EPSILON) * gain


def local_kernel(
    where_ref, x_ref, top_ref, bot_ref, left_ref, right_ref, tl_ref, tr_ref, bl_ref, br_ref,
    gain_ref, wp_ref, wo_ref, scale_ref, m1_ref, m2_ref, ggain_ref, wq_ref, gscale_ref,
    l0_ref, l1_ref, l2_ref, nx_ref, q_ref,
    pad, kk, vv, xq, qq, mask, lzero, spread,
):
    pad[3:19, 0:32, :] = x_ref[...]
    pad[0:3, 0:32, :] = top_ref[...]
    pad[19:22, 0:32, :] = bot_ref[...]
    pad[:, 32:40, :] = jnp.zeros((PAD_ROWS, 8, C0), jnp.float32)
    pad[3:19, 32:35, :] = right_ref[...]
    pad[3:19, 35:38, :] = left_ref[...]
    pad[0:3, 32:35, :] = tr_ref[...]
    pad[0:3, 35:38, :] = tl_ref[...]
    pad[19:22, 32:35, :] = br_ref[...]
    pad[19:22, 35:38, :] = bl_ref[...]
    gain = gain_ref[...]
    normed = rms(pad[...].reshape(PAD_ROWS * PAD_COLS, C0), gain)
    keys = mm(normed, wp_ref[:, C0 : 2 * C0])
    kk[...] = keys * lax.rsqrt(head_mean(keys) + EPSILON)
    vv[...] = mm(normed, wp_ref[:, 2 * C0 :])
    for half in range(2):
        spread[half] = x_ref[:, :, half * 128 : half * 128 + 128].reshape(512, 128)
    for t in range(ROWS // BLOCK):
        for n, (a1, b1, a2, b2) in enumerate(CLASSES):
            start = (BLOCK * t + 2 * a2 + a1) * COLS + 2 * b2 + b1
            for half in range(2):
                piece = spread[half, pl.ds(start, 8, stride=4), :]
                xq[t * 128 + n * 8 : t * 128 + n * 8 + 8, half * 128 : half * 128 + 128] = piece
    queries = mm(rms(xq[...], gain), wp_ref[:, :C0])
    qq[...] = queries * lax.rsqrt(head_mean(queries) + EPSILON) * scale_ref[...]

    qi = iota((128, KEYS), 0)
    ki = iota((128, KEYS), 1)
    cls = qi // 8
    q_row = 2 * ((cls // 2) % 2) + cls // 8
    q_col = 4 * (qi % 8) + 2 * (cls % 2) + (cls // 4) % 2
    slot = ki % PAD_COLS
    k_row = ki // PAD_COLS - 3
    k_col = jnp.where(slot < 35, slot, slot - 38)
    first_row = where_ref[0]
    first_col = where_ref[1]
    near = (
        (jnp.abs(k_row - q_row) <= 3)
        & (jnp.abs(k_col - q_col) <= 3)
        & (slot < 38)
        & (k_col + first_col >= 0)
        & (k_col + first_col < 512)
    )
    mask[...] = jnp.where(near, 0.0, NEG)
    lane_head = iota((128, C0), 1) // HEAD
    key_row = iota((1, KEYS), 1) // PAD_COLS - 3

    def block(t, carry):
        row = key_row + (first_row + t * BLOCK)
        bias = mask[...] + jnp.where((row >= 0) & (row < 128), 0.0, NEG)
        start = pl.multiple_of(t * (BLOCK * PAD_COLS), 8)
        k_now = kk[pl.ds(start, KEYS), :]
        v_now = vv[pl.ds(start, KEYS), :]
        q_start = pl.multiple_of(t * 128, 128)
        q_now = qq[pl.ds(q_start, 128), :]
        stacked = jnp.concatenate(
            [jnp.where(lane_head == h, q_now, 0.0) for h in range(HEADS0)], axis=0
        )
        scores = mm_t(stacked, k_now)
        weights = []
        sums = []
        for h in range(HEADS0):
            s = scores[h * 128 : (h + 1) * 128] + bias
            p = jnp.exp(s - jnp.max(s, axis=1, keepdims=True))
            weights.append(p)
            sums.append(jnp.sum(p, axis=1, keepdims=True))
        mixed = mm(jnp.concatenate(weights, axis=0), v_now)
        attended = jnp.zeros((128, C0), jnp.float32)
        for h in range(HEADS0):
            part = mixed[h * 128 : (h + 1) * 128] / sums[h]
            attended = jnp.where(lane_head == h, part, attended)
        level = xq[pl.ds(q_start, 128), :] + mm(attended, wo_ref[...])
        for n in range(16):
            at = pl.multiple_of(n * 32 + t * 8, 8)
            lzero[pl.ds(at, 8), :] = level[n * 8 : (n + 1) * 8]
        return carry

    lax.fori_loop(0, ROWS // BLOCK, block, 0)
    l0_ref[...] = lzero[...]
    one = mm(lzero[0:128, :], m1_ref[0:C0, :])
    for n in range(1, 4):
        one = one + mm(lzero[n * 128 : (n + 1) * 128, :], m1_ref[n * C0 : (n + 1) * C0, :])
    l1_ref[...] = one
    two = mm(one[0:32], m2_ref[0:CM, :])
    for n in range(1, 4):
        two = two + mm(one[n * 32 : (n + 1) * 32], m2_ref[n * CM : (n + 1) * CM, :])
    l2_ref[...] = two
    normed_two = rms(two, ggain_ref[...])
    q = mm(normed_two, wq_ref[...])
    q = q * lax.rsqrt(jnp.maximum(head_mean(q), FLOOR_VALUE)) * gscale_ref[...]
    for n in range(16):
        nx_ref[n] = normed_two
    for n in range(8):
        q_ref[n] = q


def attention_kernel(x_ref, q_ref, wk_ref, wv_ref, out_ref, kk, vv):
    x = x_ref[...].reshape(512, CG)
    keys = mm(x, wk_ref[...])
    kk[...] = keys * lax.rsqrt(jnp.maximum(head_mean(keys), FLOOR_VALUE))
    vv[...] = mm(x, wv_ref[...])
    lane_head = iota((256, 256), 1) // HEAD
    lane = iota((256, 128), 1)
    extra = jnp.zeros((256, 128), jnp.float32)
    q = q_ref[...].reshape(256, CG)
    for g in range(2):
        cols = slice(g * 256, (g + 1) * 256)
        k_now = kk[:, cols]
        v_now = vv[:, cols]
        acc = jnp.zeros((256, 256), jnp.float32)
        for h in range(4):
            s = mm_t(jnp.where(lane_head == h, q[:, cols], 0.0), k_now)
            m = jnp.max(s, axis=1, keepdims=True)
            p = jnp.exp(s - m)
            acc = jnp.where(lane_head == h, mm(p, v_now), acc)
            extra = jnp.where(lane == g * 4 + h, m, extra)
            extra = jnp.where(lane == 8 + g * 4 + h, jnp.sum(p, axis=1, keepdims=True), extra)
        out_ref[:, :, cols] = acc.reshape(8, 32, 256)
    out_ref[:, :, CG:] = extra.reshape(8, 32, 128)


def tail_kernel(part_ref, l0_ref, l1_ref, l2_ref, go_ref, s2_ref, s1_ref, out_ref, spread):
    best = part_ref[0, :, CG:]
    for n in range(1, 8):
        best = jnp.maximum(best, part_ref[n, :, CG:])
    row = iota((128, CG), 0)
    head = iota((128, CG), 1) // HEAD
    pick_weight = jnp.where(row == head, 1.0, 0.0)
    lane = iota((32, 128), 1)
    total = jnp.zeros((32, CG), jnp.float32)
    sums = jnp.zeros((32, 128), jnp.float32)
    for n in range(8):
        extra = part_ref[n, :, CG:]
        w = jnp.where(lane < 8, jnp.exp(extra - best), 0.0)
        sums = sums + w * pltpu.roll(extra, 120, 1)
        factor = jnp.dot(
            w, pick_weight, precision=lax.Precision.HIGHEST, preferred_element_type=jnp.float32
        )
        total = total + factor * part_ref[n, :, 0:CG]
    inverse = jnp.where(lane < 8, 1.0 / jnp.where(lane < 8, sums, 1.0), 0.0)
    factor = jnp.dot(
        inverse, pick_weight, precision=lax.Precision.HIGHEST, preferred_element_type=jnp.float32
    )
    mixed = l2_ref[...] + mm(total * factor, go_ref[...])
    second = mm(mixed, s2_ref[...])
    up = jnp.concatenate(
        [l1_ref[n * 32 : (n + 1) * 32, :] + second[:, n * CM : (n + 1) * CM] for n in range(4)],
        axis=0,
    )
    first = mm(up, s1_ref[...])
    for n, (a1, b1, a2, b2) in enumerate(CLASSES):
        c1 = a1 * 2 + b1
        c2 = a2 * 2 + b2
        piece = l0_ref[n * 32 : (n + 1) * 32, :] + first[
            c2 * 32 : (c2 + 1) * 32, c1 * C0 : (c1 + 1) * C0
        ]
        for i in range(4):
            start = (BLOCK * i + 2 * a2 + a1) * COLS + 2 * b2 + b1
            for half in range(2):
                spread[half, pl.ds(start, 8, stride=4), :] = piece[
                    i * 8 : (i + 1) * 8, half * 128 : half * 128 + 128
                ]
    for half in range(2):
        out_ref[:, :, half * 128 : half * 128 + 128] = spread[half].reshape(ROWS, COLS, 128)


def f32(*shape):
    return jax.ShapeDtypeStruct(shape, jnp.float32)


def shift(n, step):
    return [(i, i + step) for i in range(n) if 0 <= i + step < n]


def shards(
    latent, local_gain, local_project, local_output, local_scale, merge_first, merge_second,
    global_gain, global_project, global_output, global_scale, split_second, split_first,
):
    row_axis = ("z", "xl")
    col_axis = ("y", "xh", "c")
    both = row_axis + col_axis

    def moved(value, dr, dc):
        if dc == 0:
            return lax.ppermute(value, row_axis, shift(8, dr))
        if dr == 0:
            return lax.ppermute(value, col_axis, shift(16, dc))
        pairs = [(i * 16 + k, j * 16 + m) for i, j in shift(8, dr) for k, m in shift(16, dc)]
        return lax.ppermute(value, both, pairs)

    top = moved(latent[13:], 1, 0)
    bot = moved(latent[:3], -1, 0)
    left = moved(latent[:, 29:], 0, 1)
    right = moved(latent[:, :3], 0, -1)
    tl = moved(latent[13:, 29:], 1, 1)
    tr = moved(latent[13:, :3], 1, -1)
    bl = moved(latent[:3, 29:], -1, 1)
    br = moved(latent[:3, :3], -1, -1)
    split = global_project.reshape(CG, HEADS_G, 3, HEAD)
    wq = split[:, :, 0].reshape(CG, CG)
    wk = split[:, :, 1].reshape(CG, CG)
    wv = split[:, :, 2].reshape(CG, CG)
    where = jnp.stack([lax.axis_index(row_axis) * ROWS, lax.axis_index(col_axis) * COLS])
    scale0 = jnp.repeat(local_scale / HEAD, HEAD)[None]
    scale_g = jnp.repeat(global_scale / HEAD, HEAD)[None]
    vmem = pl.BlockSpec(memory_space=pltpu.VMEM)
    smem = pl.BlockSpec(memory_space=pltpu.SMEM)
    l0, l1, l2, nx, q = pl.pallas_call(
        local_kernel,
        out_shape=(f32(512, C0), f32(128, CM), f32(32, CG), f32(16, 32, CG), f32(8, 32, CG)),
        in_specs=[smem] + [vmem] * 18,
        out_specs=[vmem] * 5,
        scratch_shapes=[
            pltpu.VMEM((PAD_ROWS, PAD_COLS, C0), jnp.float32),
            pltpu.VMEM((PAD_ROWS * PAD_COLS, C0), jnp.float32),
            pltpu.VMEM((PAD_ROWS * PAD_COLS, C0), jnp.float32),
            pltpu.VMEM((512, C0), jnp.float32),
            pltpu.VMEM((512, C0), jnp.float32),
            pltpu.VMEM((128, KEYS), jnp.float32),
            pltpu.VMEM((512, C0), jnp.float32),
            pltpu.VMEM((2, 512, 128), jnp.float32),
        ],
        name="local",
    )(
        where, latent, top, bot, left, right, tl, tr, bl, br,
        local_gain[None], local_project, local_output, scale0, merge_first, merge_second,
        global_gain[None], wq, scale_g,
    )
    keys_from = lax.all_to_all(nx, ZX, 0, 0, tiled=True)
    queries_from = lax.all_to_all(q, YC, 0, 0, tiled=True)
    part = pl.pallas_call(
        attention_kernel,
        out_shape=f32(8, 32, CG + 128),
        in_specs=[vmem] * 4,
        out_specs=vmem,
        scratch_shapes=[pltpu.VMEM((512, CG), jnp.float32), pltpu.VMEM((512, CG), jnp.float32)],
        name="attend",
    )(keys_from, queries_from, wk, wv)
    part = lax.all_to_all(part, YC, 0, 0, tiled=True)
    return pl.pallas_call(
        tail_kernel,
        out_shape=f32(ROWS, COLS, C0),
        in_specs=[vmem] * 7,
        out_specs=vmem,
        scratch_shapes=[pltpu.VMEM((2, 512, 128), jnp.float32)],
        name="tail",
    )(part, l0, l1, l2, global_output, split_second, split_first)


def solution(mesh):
    fine = Mesh(mesh.devices.reshape(4, 2, 4, 2, 2), ("z", "xl", "y", "xh", "c"))
    tile = P(("z", "xl"), ("y", "xh", "c"), None)
    return jax.shard_map(
        shards, mesh=fine, in_specs=(tile,) + (P(),) * 12, out_specs=tile, check_vma=False
    )
```

```python
import jax
import jax.numpy as jnp
from jax import lax
from jax.experimental import pallas as pl
from jax.experimental.pallas import tpu as pltpu
from jax.sharding import Mesh, PartitionSpec as P

C0 = 256
CM = 384
CG = 512
HEADS0 = 4
HEADS_G = 8
HEAD = 64
ROWS = 16
COLS = 32
HALF = 16
BLOCK = 4
WINDOW = BLOCK + 6
SLOTS = 24
KEYS = WINDOW * SLOTS
QUERIES = BLOCK * HALF
HEIGHT = 128
BREADTH = 512
EPSILON = 1e-06
FLOOR_VALUE = 0.5
NEG = -1e30
HIGH = lax.Precision.HIGH
HIGHEST = lax.Precision.HIGHEST
BF = jnp.bfloat16
F32 = jnp.float32
ROW_AXIS = ("z", "xl")
COL_AXIS = ("y", "xh", "c")
ZX = ("z", "xh", "xl")
TURNS = (1, 3, 2)
CLASSES = [(a1, b1, a2, b2) for a1 in (0, 1) for b1 in (0, 1) for a2 in (0, 1) for b2 in (0, 1)]


def mm(a, b, precision=HIGH):
    return jnp.dot(a, b, precision=precision, preferred_element_type=F32)


def iota(shape, dim):
    return lax.broadcasted_iota(jnp.int32, shape, dim)


def parts(x):
    hi = x.astype(BF)
    return hi, (x - hi.astype(F32)).astype(BF)


def head_mean(x):
    n = x.shape[1]
    same = iota((n, n), 0) // HEAD == iota((n, n), 1) // HEAD
    weight = jnp.where(same, 1.0 / HEAD, 0.0).astype(BF)
    hi, lo = parts(x * x)
    return jnp.dot(hi, weight, preferred_element_type=F32) + jnp.dot(
        lo, weight, preferred_element_type=F32
    )


def rms(x, gain):
    return x * lax.rsqrt(jnp.mean(x * x, axis=-1, keepdims=True) + EPSILON) * gain


def unit(x):
    return x * lax.rsqrt(head_mean(x) + EPSILON)


def floored(x):
    return x * lax.rsqrt(jnp.maximum(head_mean(x), FLOOR_VALUE))


def lanes_of(ref, heads):
    lane = iota((1, heads * HEAD), 1) // HEAD
    out = jnp.zeros((1, heads * HEAD), F32)
    for h in range(heads):
        out = jnp.where(lane == h, ref[h] * (1.0 / HEAD), out)
    return out


def two_halves(x):
    hi = x.astype(BF).astype(F32)
    lo = x - hi
    return hi, lo, pltpu.roll(hi, HEAD, 1), pltpu.roll(lo, HEAD, 1)


def pair_keys(tile, first):
    hi, lo, hi_r, lo_r = two_halves(tile)
    a = jnp.concatenate([jnp.where(first, hi, hi_r), jnp.where(first, lo, lo_r)], axis=1)
    b = jnp.concatenate([jnp.where(first, hi_r, hi), jnp.where(first, lo_r, lo)], axis=1)
    return a.astype(BF), b.astype(BF)


def pair_queries(tile, first):
    hi = tile.astype(BF).astype(F32)
    lo = pltpu.roll(tile - hi, HEAD, 1)
    a = jnp.where(first, hi, lo).astype(BF)
    b = jnp.where(first, lo, hi).astype(BF)
    return jnp.concatenate([a, a], axis=1), jnp.concatenate([b, b], axis=1)


def pair_values(tile, first):
    hi = tile.astype(BF).astype(F32)
    lo = pltpu.roll(tile - hi, HEAD, 1)
    return jnp.where(first, hi, lo).astype(BF), jnp.where(first, lo, hi).astype(BF)


def scored(q, k):
    return lax.dot_general(q, k, (((1,), (1,)), ((), ())), preferred_element_type=F32)


def mixed_values(p, v):
    n = p.shape[0]
    hi, lo = parts(p)
    r = jnp.dot(jnp.concatenate([hi, lo], axis=0), v, preferred_element_type=F32)
    r = r[:n] + r[n:]
    return r + pltpu.roll(r, HEAD, 1)


def edge_kernel(x_ref, first_ref, last_ref):
    first_ref[...] = x_ref[:, 0:3, :]
    last_ref[...] = x_ref[:, COLS - 3 : COLS, :]


def row_kernel(x_ref, left_ref, right_ref, up_ref, down_ref):
    for ref, at in ((up_ref, 0), (down_ref, ROWS - 3)):
        ref[:, 0:COLS, :] = x_ref[at : at + 3]
        ref[:, COLS : COLS + 8, :] = jnp.zeros((3, 8, C0), F32)
        ref[:, COLS : COLS + 3, :] = right_ref[at : at + 3]
        ref[:, COLS + 3 : COLS + 6, :] = left_ref[at : at + 3]


def own_kernel(
    x_ref, gain_hbm, wp_hbm, scale_hbm, q_ref, k_ref, v_ref, gain, weight, scale, sems
):
    gain_in = pltpu.make_async_copy(gain_hbm, gain, sems.at[0])
    scale_in = pltpu.make_async_copy(scale_hbm, scale, sems.at[1])
    weight_in = pltpu.make_async_copy(wp_hbm, weight, sems.at[2])
    gain_in.start()
    weight_in.start()
    scale_in.start()
    gain_in.wait()
    normed = rms(x_ref[...].reshape(ROWS * COLS, C0), gain[...])
    weight_in.wait()
    q = mm(normed, weight[:, 0:C0], HIGHEST)
    scale_in.wait()
    q_ref[...] = unit(q) * lanes_of(scale, HEADS0)
    k = mm(normed, weight[:, C0 : 2 * C0], HIGHEST)
    k_ref[...] = unit(k).reshape(ROWS, COLS, C0)
    v_ref[...] = mm(normed, weight[:, 2 * C0 :]).reshape(ROWS, COLS, C0)


def keys_values(raw, gain_ref, wp_ref):
    normed = rms(raw, gain_ref[...])
    k = unit(mm(normed, wp_ref[:, C0 : 2 * C0], HIGHEST))
    return k, mm(normed, wp_ref[:, 2 * C0 :])


def windowed(own, side):
    sub = iota((1, 8, 1), 1)
    left = jnp.concatenate(
        [own[:, 0:16], jnp.where(sub < 3, own[:, 16:24], side)], axis=1
    )
    right = jnp.concatenate(
        [own[:, 16:32], jnp.where(sub >= 5, own[:, 8:16], side)], axis=1
    )
    return left, right


def near_masks(first_col):
    qi = iota((QUERIES, KEYS), 0)
    ki = iota((QUERIES, KEYS), 1)
    slot = ki % SLOTS
    row_near = jnp.abs(ki // SLOTS - 3 - qi // HALF) <= 3
    out = []
    for half in range(2):
        if half == 0:
            col = jnp.where(slot < 19, slot, slot - 22)
            real = slot < 22
        else:
            col = jnp.where(slot < 19, slot + 16, slot - 8)
            real = (slot < 19) | (slot >= 21)
        near = jnp.abs(col - (qi % HALF + half * HALF)) <= 3
        place = col + first_col
        inside = (place >= 0) & (place < BREADTH)
        out.append(jnp.where(row_near & near & real & inside, 0.0, NEG))
    return out


def window_block(q, k, v, bias, first):
    tiles = []
    for m in range(2):
        cols = slice(m * 128, (m + 1) * 128)
        queries = pair_queries(q[:, cols], first)
        keys = pair_keys(k[:, cols], first)
        values = pair_values(v[:, cols], first)
        outs = []
        for e in range(2):
            s = scored(queries[e], keys[e]) + bias
            p = jnp.exp(s - jnp.max(s, axis=1, keepdims=True))
            total = jnp.sum(p, axis=1, keepdims=True)
            outs.append(mixed_values(p, values[e]) / total)
        tiles.append(jnp.where(first, outs[0], outs[1]))
    return jnp.concatenate(tiles, axis=1)


def row_bias(first_row):
    row = iota((1, KEYS), 1) // SLOTS - 3 + first_row
    return jnp.where((row >= 0) & (row < HEIGHT), 0.0, NEG)


def places():
    return lax.axis_index(ROW_AXIS) * ROWS, lax.axis_index(COL_AXIS) * COLS


def middle_kernel(
    x_ref, left_ref, right_ref, q_ref, k_ref, v_ref, gain_ref, wp_ref, wo_ref,
    kw_ref, vw_ref, l0_ref, side,
):
    side[...] = jnp.zeros((ROWS, 8, C0), F32)
    side[:, 0:3, :] = right_ref[...]
    side[:, 3:6, :] = left_ref[...]
    k_side, v_side = keys_values(side[...].reshape(ROWS * 8, C0), gain_ref, wp_ref)
    for ref, own, extra in ((kw_ref, k_ref, k_side), (vw_ref, v_ref, v_side)):
        ref[0], ref[1] = windowed(own[...], extra.reshape(ROWS, 8, C0))
    first_row, first_col = places()
    masks = near_masks(first_col)
    first = iota((1, 128), 1) < HEAD
    for t in (1, 2):
        rows = slice(BLOCK * t, BLOCK * t + BLOCK)
        at = BLOCK * t - 3
        q = q_ref[BLOCK * t * COLS : BLOCK * (t + 1) * COLS, :].reshape(BLOCK, COLS, C0)
        outs = []
        for half in range(2):
            k = kw_ref[half, at : at + WINDOW].reshape(KEYS, C0)
            v = vw_ref[half, at : at + WINDOW].reshape(KEYS, C0)
            now = q[:, half * HALF : (half + 1) * HALF].reshape(QUERIES, C0)
            bias = masks[half] + row_bias(first_row + BLOCK * t)
            outs.append(window_block(now, k, v, bias, first).reshape(BLOCK, HALF, C0))
        attended = jnp.concatenate(outs, axis=1).reshape(BLOCK * COLS, C0)
        l0_ref[BLOCK * COLS * (t - 1) : BLOCK * COLS * t, :] = x_ref[rows].reshape(
            BLOCK * COLS, C0
        ) + mm(attended, wo_ref[...])


def outer_kernel(
    x_ref, top_ref, bot_ref, q_ref, kw_ref, vw_ref, mid_ref, gain_ref, wp_ref, wo_ref,
    m1_ref, m2_ref, ggain_ref,
    l0_ref, l1_ref, l2_ref, one_ref, nx_ref, order,
):
    raw = jnp.concatenate([top_ref[...], bot_ref[...]], axis=0).reshape(240, C0)
    k_new, v_new = keys_values(raw, gain_ref, wp_ref)
    k_new = k_new.reshape(6, 40, C0)
    v_new = v_new.reshape(6, 40, C0)
    k_new = windowed(k_new[:, 0:COLS], k_new[:, COLS:])
    v_new = windowed(v_new[:, 0:COLS], v_new[:, COLS:])
    first_row, first_col = places()
    masks = near_masks(first_col)
    first = iota((1, 128), 1) < HEAD
    for t in (0, 3):
        q = q_ref[BLOCK * t * COLS : BLOCK * (t + 1) * COLS, :].reshape(BLOCK, COLS, C0)
        outs = []
        for half in range(2):
            if t == 0:
                k = jnp.concatenate([k_new[half][0:3], kw_ref[half, 0:7]], axis=0)
                v = jnp.concatenate([v_new[half][0:3], vw_ref[half, 0:7]], axis=0)
            else:
                k = jnp.concatenate([kw_ref[half, 9:16], k_new[half][3:6]], axis=0)
                v = jnp.concatenate([vw_ref[half, 9:16], v_new[half][3:6]], axis=0)
            now = q[:, half * HALF : (half + 1) * HALF].reshape(QUERIES, C0)
            bias = masks[half] + row_bias(first_row + BLOCK * t)
            block = window_block(now, k.reshape(KEYS, C0), v.reshape(KEYS, C0), bias, first)
            outs.append(block.reshape(BLOCK, HALF, C0))
        attended = jnp.concatenate(outs, axis=1).reshape(BLOCK * COLS, C0)
        level = x_ref[BLOCK * t : BLOCK * (t + 1)].reshape(BLOCK * COLS, C0) + mm(
            attended, wo_ref[...]
        )
        for half in range(2):
            l0_ref[half, BLOCK * COLS * t : BLOCK * COLS * (t + 1), :] = level[
                :, half * 128 : (half + 1) * 128
            ]
    for half in range(2):
        l0_ref[half, 128:384, :] = mid_ref[:, half * 128 : (half + 1) * 128]
    for n, (a1, b1, a2, b2) in enumerate(CLASSES):
        for i in range(4):
            start = (BLOCK * i + 2 * a2 + a1) * COLS + 2 * b2 + b1
            for half in range(2):
                order[n * 32 + i * 8 : n * 32 + i * 8 + 8, half * 128 : half * 128 + 128] = l0_ref[
                    half, pl.ds(start, 8, stride=4), :
                ]
    one = mm(order[0:128, :], m1_ref[0:C0, :])
    for n in range(1, 4):
        one = one + mm(order[n * 128 : (n + 1) * 128, :], m1_ref[n * C0 : (n + 1) * C0, :])
    l1_ref[...] = one
    two = mm(one[0:32], m2_ref[0:CM, :])
    for n in range(1, 4):
        two = two + mm(one[n * 32 : (n + 1) * 32], m2_ref[n * CM : (n + 1) * CM, :])
    l2_ref[...] = two
    normed_two = rms(two, ggain_ref[...])
    one_ref[...] = normed_two
    for n in range(16):
        nx_ref[n] = normed_two


def chunks_in(gp_hbm, weight, sems, width):
    copies = []
    for m in range(4):
        cols = slice(384 * m, 384 * m + width)
        copies.append(pltpu.make_async_copy(gp_hbm.at[:, cols], weight.at[:, cols], sems.at[m]))
        copies[-1].start()
    return copies


def query_kernel(x_ref, gp_hbm, scale_hbm, q_ref, weight, scale, sems):
    scale_in = pltpu.make_async_copy(scale_hbm, scale, sems.at[4])
    scale_in.start()
    copies = chunks_in(gp_hbm, weight, sems, 256)
    first = iota((1, 128), 1) < HEAD
    x = x_ref[...]
    scale_in.wait()
    factor = lanes_of(scale, HEADS_G)
    for g in range(2):
        tiles = []
        for m in (2 * g, 2 * g + 1):
            copies[m].wait()
            at = 384 * m
            tiles.append(jnp.where(first, weight[:, at : at + 128], weight[:, at + 128 : at + 256]))
        q = floored(mm(x, jnp.concatenate(tiles, axis=1), HIGHEST))
        q_ref[:, g * 256 : (g + 1) * 256] = q * factor[:, g * 256 : (g + 1) * 256]


def picked(gp_ref, one, other, first):
    tiles = []
    for m in range(4):
        at = 384 * m
        a = gp_ref[:, at + 128 * one : at + 128 * one + 128]
        b = gp_ref[:, at + 128 * other : at + 128 * other + 128]
        tiles.append(jnp.where(first, a, b))
    return jnp.concatenate(tiles, axis=1)


def attention_kernel(x_ref, q_ref, gp_ref, mine_ref, other_ref, kk, vv):
    first = iota((1, 128), 1) < HEAD
    x = x_ref[...].reshape(512, CG)
    kk[...] = floored(mm(x, picked(gp_ref, 2, 0, first)))
    vv[...] = mm(x, picked(gp_ref, 1, 2, first))
    lane = iota((256, 128), 1)
    extra = jnp.zeros((256, 128), F32)
    q = q_ref[...].reshape(256, CG)
    for m in range(4):
        cols = slice(m * 128, (m + 1) * 128)
        queries = pair_queries(q[:, cols], first)
        keys = pair_keys(kk[:, cols], first)
        values = pair_values(vv[:, cols], first)
        outs = []
        for e in range(2):
            s = scored(queries[e], keys[1 - e])
            best = jnp.max(s, axis=1, keepdims=True)
            p = jnp.exp(s - best)
            outs.append(mixed_values(p, values[e]))
            extra = jnp.where(lane == 2 * m + e, best, extra)
            extra = jnp.where(lane == 8 + 2 * m + e, jnp.sum(p, axis=1, keepdims=True), extra)
        both = jnp.where(first, outs[0], outs[1]).reshape(4, 2, 32, 128)
        mine_ref[:, :, cols] = both[:, 0]
        other_ref[:, :, cols] = both[:, 1]
    both = extra.reshape(4, 2, 32, 128)
    mine_ref[:, :, CG:] = both[:, 0]
    other_ref[:, :, CG:] = both[:, 1]


def spreader():
    return jnp.where(iota((128, CG), 0) == iota((128, CG), 1) // HEAD, 1.0, 0.0)


def merge_kernel(a_ref, b_ref, *out_refs):
    a = a_ref[...].reshape(128, CG + 128)
    b = b_ref[...].reshape(128, CG + 128)
    lane = iota((128, 128), 1)
    best = jnp.maximum(a[:, CG:], b[:, CG:])
    total = jnp.zeros((128, CG), F32)
    sums = jnp.zeros((128, 128), F32)
    for part in (a, b):
        extra = part[:, CG:]
        w = jnp.where(lane < 8, jnp.exp(extra - best), 0.0)
        sums = sums + w * pltpu.roll(extra, 120, 1)
        total = total + mm(w, spreader(), HIGHEST) * part[:, 0:CG]
    extra = jnp.where(lane < 8, best, pltpu.roll(sums, 8, 1))
    for n, ref in enumerate(out_refs):
        ref[:, 0:CG] = total[n * 32 : (n + 1) * 32]
        ref[:, CG:] = extra[n * 32 : (n + 1) * 32]


def tail_kernel(
    p0_ref, p1_ref, p2_ref, p3_ref, l0_ref, l1_ref, l2_ref, go_ref, s2_ref, s1_ref, out_ref, spread
):
    arrived = (p0_ref, p1_ref, p2_ref, p3_ref)
    best = p0_ref[:, CG:]
    for ref in arrived[1:]:
        best = jnp.maximum(best, ref[:, CG:])
    pick = spreader()
    lane = iota((32, 128), 1)
    total = jnp.zeros((32, CG), F32)
    sums = jnp.zeros((32, 128), F32)
    for ref in arrived:
        extra = ref[:, CG:]
        w = jnp.where(lane < 8, jnp.exp(extra - best), 0.0)
        sums = sums + w * pltpu.roll(extra, 120, 1)
        total = total + mm(w, pick, HIGHEST) * ref[:, 0:CG]
    inverse = jnp.where(lane < 8, 1.0 / jnp.where(lane < 8, sums, 1.0), 0.0)
    mixed = l2_ref[...] + mm(total * mm(inverse, pick, HIGHEST), go_ref[...])
    second = mm(mixed, s2_ref[...])
    up = jnp.concatenate(
        [l1_ref[n * 32 : (n + 1) * 32, :] + second[:, n * CM : (n + 1) * CM] for n in range(4)],
        axis=0,
    )
    first = mm(up, s1_ref[...])
    for a1, b1, a2, b2 in CLASSES:
        c1 = a1 * 2 + b1
        c2 = a2 * 2 + b2
        for i in range(4):
            start = (BLOCK * i + 2 * a2 + a1) * COLS + 2 * b2 + b1
            for half in range(2):
                at = c1 * C0 + half * 128
                spread[half, pl.ds(start, 8, stride=4), :] = first[
                    c2 * 32 + i * 8 : c2 * 32 + i * 8 + 8, at : at + 128
                ]
    for half in range(2):
        out_ref[:, :, half * 128 : half * 128 + 128] = (spread[half] + l0_ref[half]).reshape(
            ROWS, COLS, 128
        )


def f32(*shape):
    return jax.ShapeDtypeStruct(shape, F32)


def shift(n, step):
    return [(i, i + step) for i in range(n) if 0 <= i + step < n]


V = pl.BlockSpec(memory_space=pltpu.VMEM)
H = pl.BlockSpec(memory_space=pltpu.HBM)
DMA = pltpu.SemaphoreType.DMA


def call(kernel, ins, outs, scratch=(), us=1, megabytes=16):
    many = isinstance(outs, tuple)
    run = pl.pallas_call(
        kernel,
        compiler_params=pltpu.CompilerParams(vmem_limit_bytes=megabytes << 20),
        cost_estimate=pl.CostEstimate(
            flops=int(us * 4e8), transcendentals=0, bytes_accessed=1 << 20
        ),
        out_shape=outs,
        in_specs=[H if i == "h" else V for i in ins],
        out_specs=tuple(V for _ in outs) if many else V,
        scratch_shapes=[pltpu.VMEM(s, F32) if isinstance(s, tuple) else s for s in scratch],
    )

    def placed(*args):
        return run(
            *(
                pltpu.with_memory_space_constraint(a, pltpu.HBM) if i == "h" else a
                for i, a in zip(ins, args)
            )
        )

    return placed


def shards(
    latent, local_gain, local_project, local_output, local_scale, merge_first, merge_second,
    global_gain, global_project, global_output, global_scale, split_second, split_first,
):
    gain = local_gain[None]
    first, last = call(edge_kernel, "v", (f32(ROWS, 3, C0), f32(ROWS, 3, C0)))(latent)
    right = lax.ppermute(first, COL_AXIS, shift(16, -1))
    left = lax.ppermute(last, COL_AXIS, shift(16, 1))
    q, k, v = call(
        own_kernel,
        "vhhh",
        (f32(512, C0), f32(ROWS, COLS, C0), f32(ROWS, COLS, C0)),
        [(1, C0), (C0, 3 * C0), pltpu.SMEM((HEADS0,), F32), DMA((3,))],
        us=5,
    )(latent, gain, local_project, local_scale)
    up, down = call(row_kernel, "vvv", (f32(3, 40, C0), f32(3, 40, C0)))(latent, left, right)
    bot = lax.ppermute(up, ROW_AXIS, shift(8, -1))
    top = lax.ppermute(down, ROW_AXIS, shift(8, 1))
    kw, vw, mid = call(
        middle_kernel,
        "v" * 9,
        (f32(2, ROWS, SLOTS, C0), f32(2, ROWS, SLOTS, C0), f32(256, C0)),
        [(ROWS, 8, C0)],
        us=8,
    )(latent, left, right, q, k, v, gain, local_project, local_output)
    l0, l1, l2, one, nx = call(
        outer_kernel,
        "v" * 13,
        (f32(2, 512, 128), f32(128, CM), f32(32, CG), f32(32, CG), f32(16, 32, CG)),
        [(512, C0)],
    )(
        latent, top, bot, q, kw, vw, mid, gain, local_project, local_output,
        merge_first, merge_second, global_gain[None],
    )
    keys_from = lax.all_to_all(nx, ZX, 0, 0, tiled=True)
    qg = call(
        query_kernel,
        "vhh",
        f32(32, CG),
        [(CG, 3 * CG), pltpu.SMEM((HEADS_G,), F32), DMA((5,))],
        us=4,
    )(one, global_project, global_scale)
    swapped = lax.ppermute(qg, "c", [(0, 1), (1, 0)])
    two = jnp.stack([qg, swapped])
    around = [lax.ppermute(two, "y", [(i, (i + d) % 4) for i in range(4)]) for d in TURNS]
    queries_from = jnp.concatenate([two] + around)
    mine, other = call(
        attention_kernel,
        "vvv",
        (f32(4, 32, CG + 128), f32(4, 32, CG + 128)),
        [(512, CG), (512, CG)],
    )(keys_from, queries_from, global_project)
    theirs = lax.ppermute(other, "c", [(0, 1), (1, 0)])
    merged = call(merge_kernel, "vv", tuple(f32(32, CG + 128) for _ in range(4)))(mine, theirs)
    arrived = [merged[0]] + [
        lax.ppermute(part, "y", [(i, (i - d) % 4) for i in range(4)])
        for part, d in zip(merged[1:], TURNS)
    ]
    return call(tail_kernel, "v" * 10, f32(ROWS, COLS, C0), [(2, 512, 128)])(
        *arrived, l0, l1, l2, global_output, split_second, split_first
    )


def solution(mesh):
    fine = Mesh(mesh.devices.reshape(4, 2, 4, 2, 2), ("z", "xl", "y", "xh", "c"))
    tile = P(ROW_AXIS, COL_AXIS, None)
    return jax.shard_map(
        shards, mesh=fine, in_specs=(tile,) + (P(),) * 12, out_specs=tile, check_vma=False
    )
```

```python
import jax
import jax.numpy as jnp
from jax import lax
from jax.experimental import pallas as pl
from jax.experimental.pallas import tpu as pltpu
from jax.sharding import Mesh, PartitionSpec as P

C0 = 256
CM = 384
CG = 512
HEADS0 = 4
HEADS_G = 8
HEAD = 64
ROWS = 16
COLS = 32
HALF = 16
BLOCK = 4
WINDOW = BLOCK + 6
SLOTS = 24
KEYS = WINDOW * SLOTS
QUERIES = BLOCK * HALF
HEIGHT = 128
BREADTH = 512
EPSILON = 1e-06
FLOOR_VALUE = 0.5
NEG = -1e30
HIGH = lax.Precision.HIGH
HIGHEST = lax.Precision.HIGHEST
BF = jnp.bfloat16
F32 = jnp.float32
ROW_AXIS = ("z", "xl")
COL_AXIS = ("y", "xh", "c")
ZX = ("z", "xh", "xl")
TURNS = (1, 3, 2)
CLASSES = [(a1, b1, a2, b2) for a1 in (0, 1) for b1 in (0, 1) for a2 in (0, 1) for b2 in (0, 1)]


def mm(a, b, precision=HIGH):
    return jnp.dot(a, b, precision=precision, preferred_element_type=F32)


def iota(shape, dim):
    return lax.broadcasted_iota(jnp.int32, shape, dim)


def parts(x):
    hi = x.astype(BF)
    return hi, (x - hi.astype(F32)).astype(BF)


def head_mean(x):
    n = x.shape[1]
    same = iota((n, n), 0) // HEAD == iota((n, n), 1) // HEAD
    weight = jnp.where(same, 1.0 / HEAD, 0.0).astype(BF)
    hi, lo = parts(x * x)
    return jnp.dot(hi, weight, preferred_element_type=F32) + jnp.dot(
        lo, weight, preferred_element_type=F32
    )


def rms(x, gain):
    return x * lax.rsqrt(jnp.mean(x * x, axis=-1, keepdims=True) + EPSILON) * gain


def unit(x):
    return x * lax.rsqrt(head_mean(x) + EPSILON)


def floored(x):
    return x * lax.rsqrt(jnp.maximum(head_mean(x), FLOOR_VALUE))


def lanes_of(ref, heads):
    lane = iota((1, heads * HEAD), 1) // HEAD
    out = jnp.zeros((1, heads * HEAD), F32)
    for h in range(heads):
        out = jnp.where(lane == h, ref[h] * (1.0 / HEAD), out)
    return out


def two_halves(x):
    hi = x.astype(BF).astype(F32)
    lo = x - hi
    return hi, lo, pltpu.roll(hi, HEAD, 1), pltpu.roll(lo, HEAD, 1)


def pair_keys(tile, first):
    hi, lo, hi_r, lo_r = two_halves(tile)
    a = jnp.concatenate([jnp.where(first, hi, hi_r), jnp.where(first, lo, lo_r)], axis=1)
    b = jnp.concatenate([jnp.where(first, hi_r, hi), jnp.where(first, lo_r, lo)], axis=1)
    return a.astype(BF), b.astype(BF)


def pair_queries(tile, first):
    hi = tile.astype(BF).astype(F32)
    lo = pltpu.roll(tile - hi, HEAD, 1)
    a = jnp.where(first, hi, lo).astype(BF)
    b = jnp.where(first, lo, hi).astype(BF)
    return jnp.concatenate([a, a], axis=1), jnp.concatenate([b, b], axis=1)


def pair_values(tile, first):
    hi = tile.astype(BF).astype(F32)
    lo = pltpu.roll(tile - hi, HEAD, 1)
    return jnp.where(first, hi, lo).astype(BF), jnp.where(first, lo, hi).astype(BF)


def scored(q, k):
    return lax.dot_general(q, k, (((1,), (1,)), ((), ())), preferred_element_type=F32)


def mixed_values(p, v):
    n = p.shape[0]
    hi, lo = parts(p)
    r = jnp.dot(jnp.concatenate([hi, lo], axis=0), v, preferred_element_type=F32)
    r = r[:n] + r[n:]
    return r + pltpu.roll(r, HEAD, 1)


def edge_kernel(x_ref, inner_ref, outer_ref):
    even = lax.axis_index("c") == 0
    first = x_ref[:, 0:3, :]
    last = x_ref[:, COLS - 3 : COLS, :]
    inner_ref[...] = jnp.where(even, last, first)
    outer_ref[...] = jnp.where(even, first, last)


def sides(inner_ref, outer_ref):
    even = lax.axis_index("c") == 0
    inner = inner_ref[...]
    outer = outer_ref[...]
    return jnp.where(even, outer, inner), jnp.where(even, inner, outer)


def row_kernel(x_ref, in_ref, out_ref, inner_ref, outer_ref):
    left, right = sides(in_ref, out_ref)
    even = lax.axis_index("xl") == 0
    x_first = x_ref[0:3]
    x_last = x_ref[ROWS - 3 : ROWS]
    for ref, down in ((inner_ref, even), (outer_ref, jnp.logical_not(even))):
        ref[:, 0:COLS, :] = jnp.where(down, x_last, x_first)
        ref[:, COLS : COLS + 8, :] = jnp.zeros((3, 8, C0), F32)
        ref[:, COLS : COLS + 3, :] = jnp.where(down, right[ROWS - 3 :], right[0:3])
        ref[:, COLS + 3 : COLS + 6, :] = jnp.where(down, left[ROWS - 3 :], left[0:3])


def own_kernel(
    x_ref, gain_hbm, wp_hbm, scale_hbm, q_ref, k_ref, v_ref, gain, weight, scale, sems
):
    gain_in = pltpu.make_async_copy(gain_hbm, gain, sems.at[0])
    scale_in = pltpu.make_async_copy(scale_hbm, scale, sems.at[1])
    weight_in = pltpu.make_async_copy(wp_hbm, weight, sems.at[2])
    gain_in.start()
    weight_in.start()
    scale_in.start()
    gain_in.wait()
    normed = rms(x_ref[...].reshape(ROWS * COLS, C0), gain[...])
    weight_in.wait()
    q = mm(normed, weight[:, 0:C0], HIGHEST)
    scale_in.wait()
    q_ref[...] = unit(q) * lanes_of(scale, HEADS0)
    k = mm(normed, weight[:, C0 : 2 * C0], HIGHEST)
    k_ref[...] = unit(k).reshape(ROWS, COLS, C0)
    v_ref[...] = mm(normed, weight[:, 2 * C0 :]).reshape(ROWS, COLS, C0)


def keys_values(raw, gain_ref, wp_ref):
    normed = rms(raw, gain_ref[...])
    k = unit(mm(normed, wp_ref[:, C0 : 2 * C0], HIGHEST))
    return k, mm(normed, wp_ref[:, 2 * C0 :])


def windowed(own, side):
    sub = iota((1, 8, 1), 1)
    left = jnp.concatenate(
        [own[:, 0:16], jnp.where(sub < 3, own[:, 16:24], side)], axis=1
    )
    right = jnp.concatenate(
        [own[:, 16:32], jnp.where(sub >= 5, own[:, 8:16], side)], axis=1
    )
    return left, right


def near_masks(first_col):
    qi = iota((QUERIES, KEYS), 0)
    ki = iota((QUERIES, KEYS), 1)
    slot = ki % SLOTS
    row_near = jnp.abs(ki // SLOTS - 3 - qi // HALF) <= 3
    out = []
    for half in range(2):
        if half == 0:
            col = jnp.where(slot < 19, slot, slot - 22)
            real = slot < 22
        else:
            col = jnp.where(slot < 19, slot + 16, slot - 8)
            real = (slot < 19) | (slot >= 21)
        near = jnp.abs(col - (qi % HALF + half * HALF)) <= 3
        place = col + first_col
        inside = (place >= 0) & (place < BREADTH)
        out.append(jnp.where(row_near & near & real & inside, 0.0, NEG))
    return out


def window_block(q, k, v, bias, first):
    tiles = []
    for m in range(2):
        cols = slice(m * 128, (m + 1) * 128)
        queries = pair_queries(q[:, cols], first)
        keys = pair_keys(k[:, cols], first)
        values = pair_values(v[:, cols], first)
        outs = []
        for e in range(2):
            s = scored(queries[e], keys[e]) + bias
            p = jnp.exp(s - jnp.max(s, axis=1, keepdims=True))
            total = jnp.sum(p, axis=1, keepdims=True)
            outs.append(mixed_values(p, values[e]) / total)
        tiles.append(jnp.where(first, outs[0], outs[1]))
    return jnp.concatenate(tiles, axis=1)


def row_bias(first_row):
    row = iota((1, KEYS), 1) // SLOTS - 3 + first_row
    return jnp.where((row >= 0) & (row < HEIGHT), 0.0, NEG)


def places():
    return lax.axis_index(ROW_AXIS) * ROWS, lax.axis_index(COL_AXIS) * COLS


def middle_kernel(
    x_ref, in_ref, out_ref, q_ref, k_ref, v_ref, gain_ref, wp_ref, wo_ref,
    kw_ref, vw_ref, l0_ref, side,
):
    side[...] = jnp.zeros((ROWS, 8, C0), F32)
    left, right = sides(in_ref, out_ref)
    side[:, 0:3, :] = right
    side[:, 3:6, :] = left
    k_side, v_side = keys_values(side[...].reshape(ROWS * 8, C0), gain_ref, wp_ref)
    for ref, own, extra in ((kw_ref, k_ref, k_side), (vw_ref, v_ref, v_side)):
        ref[0], ref[1] = windowed(own[...], extra.reshape(ROWS, 8, C0))
    first_row, first_col = places()
    masks = near_masks(first_col)
    first = iota((1, 128), 1) < HEAD
    for t in (1, 2):
        rows = slice(BLOCK * t, BLOCK * t + BLOCK)
        at = BLOCK * t - 3
        q = q_ref[BLOCK * t * COLS : BLOCK * (t + 1) * COLS, :].reshape(BLOCK, COLS, C0)
        outs = []
        for half in range(2):
            k = kw_ref[half, at : at + WINDOW].reshape(KEYS, C0)
            v = vw_ref[half, at : at + WINDOW].reshape(KEYS, C0)
            now = q[:, half * HALF : (half + 1) * HALF].reshape(QUERIES, C0)
            bias = masks[half] + row_bias(first_row + BLOCK * t)
            outs.append(window_block(now, k, v, bias, first).reshape(BLOCK, HALF, C0))
        attended = jnp.concatenate(outs, axis=1).reshape(BLOCK * COLS, C0)
        l0_ref[BLOCK * COLS * (t - 1) : BLOCK * COLS * t, :] = x_ref[rows].reshape(
            BLOCK * COLS, C0
        ) + mm(attended, wo_ref[...])


def outer_kernel(
    x_ref, in_ref, out_ref, q_ref, kw_ref, vw_ref, mid_ref, gain_ref, wp_ref, wo_ref,
    m1_ref, m2_ref, ggain_ref,
    l0_ref, l1_ref, l2_ref, one_ref, nx_ref, order,
):
    even = lax.axis_index("xl") == 0
    top = jnp.where(even, out_ref[...], in_ref[...])
    bot = jnp.where(even, in_ref[...], out_ref[...])
    raw = jnp.concatenate([top, bot], axis=0).reshape(240, C0)
    k_new, v_new = keys_values(raw, gain_ref, wp_ref)
    k_new = k_new.reshape(6, 40, C0)
    v_new = v_new.reshape(6, 40, C0)
    k_new = windowed(k_new[:, 0:COLS], k_new[:, COLS:])
    v_new = windowed(v_new[:, 0:COLS], v_new[:, COLS:])
    first_row, first_col = places()
    masks = near_masks(first_col)
    first = iota((1, 128), 1) < HEAD
    for t in (0, 3):
        q = q_ref[BLOCK * t * COLS : BLOCK * (t + 1) * COLS, :].reshape(BLOCK, COLS, C0)
        outs = []
        for half in range(2):
            if t == 0:
                k = jnp.concatenate([k_new[half][0:3], kw_ref[half, 0:7]], axis=0)
                v = jnp.concatenate([v_new[half][0:3], vw_ref[half, 0:7]], axis=0)
            else:
                k = jnp.concatenate([kw_ref[half, 9:16], k_new[half][3:6]], axis=0)
                v = jnp.concatenate([vw_ref[half, 9:16], v_new[half][3:6]], axis=0)
            now = q[:, half * HALF : (half + 1) * HALF].reshape(QUERIES, C0)
            bias = masks[half] + row_bias(first_row + BLOCK * t)
            block = window_block(now, k.reshape(KEYS, C0), v.reshape(KEYS, C0), bias, first)
            outs.append(block.reshape(BLOCK, HALF, C0))
        attended = jnp.concatenate(outs, axis=1).reshape(BLOCK * COLS, C0)
        level = x_ref[BLOCK * t : BLOCK * (t + 1)].reshape(BLOCK * COLS, C0) + mm(
            attended, wo_ref[...]
        )
        for half in range(2):
            l0_ref[half, BLOCK * COLS * t : BLOCK * COLS * (t + 1), :] = level[
                :, half * 128 : (half + 1) * 128
            ]
    for half in range(2):
        l0_ref[half, 128:384, :] = mid_ref[:, half * 128 : (half + 1) * 128]
    for n, (a1, b1, a2, b2) in enumerate(CLASSES):
        for i in range(4):
            start = (BLOCK * i + 2 * a2 + a1) * COLS + 2 * b2 + b1
            for half in range(2):
                order[n * 32 + i * 8 : n * 32 + i * 8 + 8, half * 128 : half * 128 + 128] = l0_ref[
                    half, pl.ds(start, 8, stride=4), :
                ]
    one = mm(order[0:128, :], m1_ref[0:C0, :])
    for n in range(1, 4):
        one = one + mm(order[n * 128 : (n + 1) * 128, :], m1_ref[n * C0 : (n + 1) * C0, :])
    l1_ref[...] = one
    two = mm(one[0:32], m2_ref[0:CM, :])
    for n in range(1, 4):
        two = two + mm(one[n * 32 : (n + 1) * 32], m2_ref[n * CM : (n + 1) * CM, :])
    l2_ref[...] = two
    normed_two = rms(two, ggain_ref[...])
    one_ref[...] = normed_two
    for n in range(16):
        nx_ref[n] = normed_two


def chunks_in(gp_hbm, weight, sems, width):
    copies = []
    for m in range(4):
        cols = slice(384 * m, 384 * m + width)
        copies.append(pltpu.make_async_copy(gp_hbm.at[:, cols], weight.at[:, cols], sems.at[m]))
        copies[-1].start()
    return copies


def query_kernel(x_ref, gp_hbm, scale_hbm, q_ref, weight, scale, sems):
    scale_in = pltpu.make_async_copy(scale_hbm, scale, sems.at[4])
    scale_in.start()
    copies = chunks_in(gp_hbm, weight, sems, 256)
    first = iota((1, 128), 1) < HEAD
    x = x_ref[...]
    scale_in.wait()
    factor = lanes_of(scale, HEADS_G)
    for g in range(2):
        tiles = []
        for m in (2 * g, 2 * g + 1):
            copies[m].wait()
            at = 384 * m
            tiles.append(jnp.where(first, weight[:, at : at + 128], weight[:, at + 128 : at + 256]))
        q = floored(mm(x, jnp.concatenate(tiles, axis=1), HIGHEST))
        q_ref[:, g * 256 : (g + 1) * 256] = q * factor[:, g * 256 : (g + 1) * 256]


def picked(gp_ref, one, other, first):
    tiles = []
    for m in range(4):
        at = 384 * m
        a = gp_ref[:, at + 128 * one : at + 128 * one + 128]
        b = gp_ref[:, at + 128 * other : at + 128 * other + 128]
        tiles.append(jnp.where(first, a, b))
    return jnp.concatenate(tiles, axis=1)


def attention_kernel(x_ref, q_ref, gp_ref, mine_ref, other_ref, kk, vv):
    first = iota((1, 128), 1) < HEAD
    x = x_ref[...].reshape(512, CG)
    kk[...] = floored(mm(x, picked(gp_ref, 2, 0, first)))
    vv[...] = mm(x, picked(gp_ref, 1, 2, first))
    lane = iota((256, 128), 1)
    extra = jnp.zeros((256, 128), F32)
    q = q_ref[...].reshape(256, CG)
    for m in range(4):
        cols = slice(m * 128, (m + 1) * 128)
        queries = pair_queries(q[:, cols], first)
        keys = pair_keys(kk[:, cols], first)
        values = pair_values(vv[:, cols], first)
        outs = []
        for e in range(2):
            s = scored(queries[e], keys[1 - e])
            best = jnp.max(s, axis=1, keepdims=True)
            p = jnp.exp(s - best)
            outs.append(mixed_values(p, values[e]))
            extra = jnp.where(lane == 2 * m + e, best, extra)
            extra = jnp.where(lane == 8 + 2 * m + e, jnp.sum(p, axis=1, keepdims=True), extra)
        both = jnp.where(first, outs[0], outs[1]).reshape(4, 2, 32, 128)
        mine_ref[:, :, cols] = both[:, 0]
        other_ref[:, :, cols] = both[:, 1]
    both = extra.reshape(4, 2, 32, 128)
    mine_ref[:, :, CG:] = both[:, 0]
    other_ref[:, :, CG:] = both[:, 1]


def spreader():
    return jnp.where(iota((128, CG), 0) == iota((128, CG), 1) // HEAD, 1.0, 0.0)


def merge_kernel(a_ref, b_ref, *out_refs):
    a = a_ref[...].reshape(128, CG + 128)
    b = b_ref[...].reshape(128, CG + 128)
    lane = iota((128, 128), 1)
    best = jnp.maximum(a[:, CG:], b[:, CG:])
    total = jnp.zeros((128, CG), F32)
    sums = jnp.zeros((128, 128), F32)
    for part in (a, b):
        extra = part[:, CG:]
        w = jnp.where(lane < 8, jnp.exp(extra - best), 0.0)
        sums = sums + w * pltpu.roll(extra, 120, 1)
        total = total + mm(w, spreader(), HIGHEST) * part[:, 0:CG]
    extra = jnp.where(lane < 8, best, pltpu.roll(sums, 8, 1))
    for n, ref in enumerate(out_refs):
        ref[:, 0:CG] = total[n * 32 : (n + 1) * 32]
        ref[:, CG:] = extra[n * 32 : (n + 1) * 32]


def tail_kernel(
    p0_ref, p1_ref, p2_ref, p3_ref, l0_ref, l1_ref, l2_ref, go_ref, s2_ref, s1_ref, out_ref, spread
):
    arrived = (p0_ref, p1_ref, p2_ref, p3_ref)
    best = p0_ref[:, CG:]
    for ref in arrived[1:]:
        best = jnp.maximum(best, ref[:, CG:])
    pick = spreader()
    lane = iota((32, 128), 1)
    total = jnp.zeros((32, CG), F32)
    sums = jnp.zeros((32, 128), F32)
    for ref in arrived:
        extra = ref[:, CG:]
        w = jnp.where(lane < 8, jnp.exp(extra - best), 0.0)
        sums = sums + w * pltpu.roll(extra, 120, 1)
        total = total + mm(w, pick, HIGHEST) * ref[:, 0:CG]
    inverse = jnp.where(lane < 8, 1.0 / jnp.where(lane < 8, sums, 1.0), 0.0)
    mixed = l2_ref[...] + mm(total * mm(inverse, pick, HIGHEST), go_ref[...])
    second = mm(mixed, s2_ref[...])
    up = jnp.concatenate(
        [l1_ref[n * 32 : (n + 1) * 32, :] + second[:, n * CM : (n + 1) * CM] for n in range(4)],
        axis=0,
    )
    first = mm(up, s1_ref[...])
    for a1, b1, a2, b2 in CLASSES:
        c1 = a1 * 2 + b1
        c2 = a2 * 2 + b2
        for i in range(4):
            start = (BLOCK * i + 2 * a2 + a1) * COLS + 2 * b2 + b1
            for half in range(2):
                at = c1 * C0 + half * 128
                spread[half, pl.ds(start, 8, stride=4), :] = first[
                    c2 * 32 + i * 8 : c2 * 32 + i * 8 + 8, at : at + 128
                ]
    for half in range(2):
        out_ref[:, :, half * 128 : half * 128 + 128] = (spread[half] + l0_ref[half]).reshape(
            ROWS, COLS, 128
        )


def f32(*shape):
    return jax.ShapeDtypeStruct(shape, F32)


def odd_swaps(n):
    return [p for i in range(1, n - 1, 2) for p in ((i, i + 1), (i + 1, i))]


V = pl.BlockSpec(memory_space=pltpu.VMEM)
H = pl.BlockSpec(memory_space=pltpu.HBM)
DMA = pltpu.SemaphoreType.DMA


def call(kernel, ins, outs, scratch=(), us=1, megabytes=16):
    many = isinstance(outs, tuple)
    run = pl.pallas_call(
        kernel,
        compiler_params=pltpu.CompilerParams(vmem_limit_bytes=megabytes << 20),
        cost_estimate=pl.CostEstimate(
            flops=int(us * 4e8), transcendentals=0, bytes_accessed=1 << 20
        ),
        out_shape=outs,
        in_specs=[H if i == "h" else V for i in ins],
        out_specs=tuple(V for _ in outs) if many else V,
        scratch_shapes=[pltpu.VMEM(s, F32) if isinstance(s, tuple) else s for s in scratch],
    )

    def placed(*args):
        return run(
            *(
                pltpu.with_memory_space_constraint(a, pltpu.HBM) if i == "h" else a
                for i, a in zip(ins, args)
            )
        )

    return placed


def shards(
    latent, local_gain, local_project, local_output, local_scale, merge_first, merge_second,
    global_gain, global_project, global_output, global_scale, split_second, split_first,
):
    gain = local_gain[None]
    inner, outer = call(edge_kernel, "v", (f32(ROWS, 3, C0), f32(ROWS, 3, C0)))(latent)
    col_in = lax.ppermute(inner, "c", [(0, 1), (1, 0)])
    col_out = lax.ppermute(outer, COL_AXIS, odd_swaps(16))
    q, k, v = call(
        own_kernel,
        "vhhh",
        (f32(512, C0), f32(ROWS, COLS, C0), f32(ROWS, COLS, C0)),
        [(1, C0), (C0, 3 * C0), pltpu.SMEM((HEADS0,), F32), DMA((3,))],
        us=5,
    )(latent, gain, local_project, local_scale)
    inner, outer = call(row_kernel, "vvv", (f32(3, 40, C0), f32(3, 40, C0)))(
        latent, col_in, col_out
    )
    row_in = lax.ppermute(inner, "xl", [(0, 1), (1, 0)])
    row_out = lax.ppermute(outer, ROW_AXIS, odd_swaps(8))
    kw, vw, mid = call(
        middle_kernel,
        "v" * 9,
        (f32(2, ROWS, SLOTS, C0), f32(2, ROWS, SLOTS, C0), f32(256, C0)),
        [(ROWS, 8, C0)],
        us=8,
    )(latent, col_in, col_out, q, k, v, gain, local_project, local_output)
    l0, l1, l2, one, nx = call(
        outer_kernel,
        "v" * 13,
        (f32(2, 512, 128), f32(128, CM), f32(32, CG), f32(32, CG), f32(16, 32, CG)),
        [(512, C0)],
    )(
        latent, row_in, row_out, q, kw, vw, mid, gain, local_project, local_output,
        merge_first, merge_second, global_gain[None],
    )
    keys_from = lax.all_to_all(nx, ZX, 0, 0, tiled=True)
    qg = call(
        query_kernel,
        "vhh",
        f32(32, CG),
        [(CG, 3 * CG), pltpu.SMEM((HEADS_G,), F32), DMA((5,))],
        us=4,
    )(one, global_project, global_scale)
    swapped = lax.ppermute(qg, "c", [(0, 1), (1, 0)])
    two = jnp.stack([qg, swapped])
    around = [lax.ppermute(two, "y", [(i, (i + d) % 4) for i in range(4)]) for d in TURNS]
    queries_from = jnp.concatenate([two] + around)
    mine, other = call(
        attention_kernel,
        "vvv",
        (f32(4, 32, CG + 128), f32(4, 32, CG + 128)),
        [(512, CG), (512, CG)],
    )(keys_from, queries_from, global_project)
    theirs = lax.ppermute(other, "c", [(0, 1), (1, 0)])
    merged = call(merge_kernel, "vv", tuple(f32(32, CG + 128) for _ in range(4)))(mine, theirs)
    arrived = [merged[0]] + [
        lax.ppermute(part, "y", [(i, (i - d) % 4) for i in range(4)])
        for part, d in zip(merged[1:], TURNS)
    ]
    return call(tail_kernel, "v" * 10, f32(ROWS, COLS, C0), [(2, 512, 128)])(
        *arrived, l0, l1, l2, global_output, split_second, split_first
    )


def solution(mesh):
    fine = Mesh(mesh.devices.reshape(4, 2, 4, 2, 2), ("z", "xl", "y", "xh", "c"))
    tile = P(ROW_AXIS, COL_AXIS, None)
    return jax.shard_map(
        shards, mesh=fine, in_specs=(tile,) + (P(),) * 12, out_specs=tile, check_vma=False
    )
```

```python
import jax
import jax.numpy as jnp
from jax import lax
from jax.experimental import pallas as pl
from jax.experimental.pallas import tpu as pltpu
from jax.sharding import Mesh, PartitionSpec as P

C0 = 256
CM = 384
CG = 512
HEADS0 = 4
HEADS_G = 8
HEAD = 64
ROWS = 16
COLS = 32
HALF = 16
BLOCK = 4
WINDOW = BLOCK + 6
SLOTS = 24
KEYS = WINDOW * SLOTS
QUERIES = BLOCK * HALF
HEIGHT = 128
BREADTH = 512
EPSILON = 1e-06
FLOOR_VALUE = 0.5
NEG = -1e30
HIGH = lax.Precision.HIGH
HIGHEST = lax.Precision.HIGHEST
BF = jnp.bfloat16
F32 = jnp.float32
ROW_AXIS = ("z", "xl")
COL_AXIS = ("y", "xh", "c")
TURNS = (1, 3, 2)
CLASSES = [(a1, b1, a2, b2) for a1 in (0, 1) for b1 in (0, 1) for a2 in (0, 1) for b2 in (0, 1)]


def mm(a, b, precision=HIGH):
    return jnp.dot(a, b, precision=precision, preferred_element_type=F32)


def iota(shape, dim):
    return lax.broadcasted_iota(jnp.int32, shape, dim)


def parts(x):
    hi = x.astype(BF)
    return hi, (x - hi.astype(F32)).astype(BF)


def head_mean(x):
    n = x.shape[1]
    same = iota((n, n), 0) // HEAD == iota((n, n), 1) // HEAD
    weight = jnp.where(same, 1.0 / HEAD, 0.0).astype(BF)
    hi, lo = parts(x * x)
    return jnp.dot(hi, weight, preferred_element_type=F32) + jnp.dot(
        lo, weight, preferred_element_type=F32
    )


def rms(x, gain):
    return x * lax.rsqrt(jnp.mean(x * x, axis=-1, keepdims=True) + EPSILON) * gain


def unit(x):
    return x * lax.rsqrt(head_mean(x) + EPSILON)


def floored(x):
    return x * lax.rsqrt(jnp.maximum(head_mean(x), FLOOR_VALUE))


def lanes_of(ref, heads):
    lane = iota((1, heads * HEAD), 1) // HEAD
    out = jnp.zeros((1, heads * HEAD), F32)
    for h in range(heads):
        out = jnp.where(lane == h, ref[h] * (1.0 / HEAD), out)
    return out


def two_halves(x):
    hi = x.astype(BF).astype(F32)
    lo = x - hi
    return hi, lo, pltpu.roll(hi, HEAD, 1), pltpu.roll(lo, HEAD, 1)


def pair_keys(tile, first):
    hi, lo, hi_r, lo_r = two_halves(tile)
    a = jnp.concatenate([jnp.where(first, hi, hi_r), jnp.where(first, lo, lo_r)], axis=1)
    b = jnp.concatenate([jnp.where(first, hi_r, hi), jnp.where(first, lo_r, lo)], axis=1)
    return a.astype(BF), b.astype(BF)


def pair_queries(tile, first):
    hi = tile.astype(BF).astype(F32)
    lo = pltpu.roll(tile - hi, HEAD, 1)
    a = jnp.where(first, hi, lo).astype(BF)
    b = jnp.where(first, lo, hi).astype(BF)
    return jnp.concatenate([a, a], axis=1), jnp.concatenate([b, b], axis=1)


def pair_values(tile, first):
    hi = tile.astype(BF).astype(F32)
    lo = pltpu.roll(tile - hi, HEAD, 1)
    return jnp.where(first, hi, lo).astype(BF), jnp.where(first, lo, hi).astype(BF)


def scored(q, k):
    return lax.dot_general(q, k, (((1,), (1,)), ((), ())), preferred_element_type=F32)


def mixed_values(p, v):
    n = p.shape[0]
    hi, lo = parts(p)
    r = jnp.dot(jnp.concatenate([hi, lo], axis=0), v, preferred_element_type=F32)
    r = r[:n] + r[n:]
    return r + pltpu.roll(r, HEAD, 1)


def edge_kernel(x_ref, inner_ref, outer_ref):
    even = lax.axis_index("c") == 0
    first = x_ref[:, 0:3, :]
    last = x_ref[:, COLS - 3 : COLS, :]
    inner_ref[...] = jnp.where(even, last, first)
    outer_ref[...] = jnp.where(even, first, last)


def sides(inner_ref, outer_ref):
    even = lax.axis_index("c") == 0
    inner = inner_ref[...]
    outer = outer_ref[...]
    return jnp.where(even, outer, inner), jnp.where(even, inner, outer)


def row_kernel(x_ref, in_ref, out_ref, inner_ref, outer_ref):
    left, right = sides(in_ref, out_ref)
    even = lax.axis_index("xl") == 0
    x_first = x_ref[0:3]
    x_last = x_ref[ROWS - 3 : ROWS]
    for ref, down in ((inner_ref, even), (outer_ref, jnp.logical_not(even))):
        ref[:, 0:COLS, :] = jnp.where(down, x_last, x_first)
        ref[:, COLS : COLS + 8, :] = jnp.zeros((3, 8, C0), F32)
        ref[:, COLS : COLS + 3, :] = jnp.where(down, right[ROWS - 3 :], right[0:3])
        ref[:, COLS + 3 : COLS + 6, :] = jnp.where(down, left[ROWS - 3 :], left[0:3])


def own_kernel(
    x_ref, gain_hbm, wp_hbm, scale_hbm, q_ref, k_ref, v_ref, gain, weight, scale, sems
):
    gain_in = pltpu.make_async_copy(gain_hbm, gain, sems.at[0])
    scale_in = pltpu.make_async_copy(scale_hbm, scale, sems.at[1])
    weight_in = pltpu.make_async_copy(wp_hbm, weight, sems.at[2])
    gain_in.start()
    weight_in.start()
    scale_in.start()
    gain_in.wait()
    normed = rms(x_ref[...].reshape(ROWS * COLS, C0), gain[...])
    weight_in.wait()
    q = mm(normed, weight[:, 0:C0], HIGHEST)
    scale_in.wait()
    q_ref[...] = unit(q) * lanes_of(scale, HEADS0)
    k = mm(normed, weight[:, C0 : 2 * C0], HIGHEST)
    k_ref[...] = unit(k).reshape(ROWS, COLS, C0)
    v_ref[...] = mm(normed, weight[:, 2 * C0 :]).reshape(ROWS, COLS, C0)


def keys_values(raw, gain_ref, wp_ref):
    normed = rms(raw, gain_ref[...])
    k = unit(mm(normed, wp_ref[:, C0 : 2 * C0], HIGHEST))
    return k, mm(normed, wp_ref[:, 2 * C0 :])


def windowed(own, side):
    sub = iota((1, 8, 1), 1)
    left = jnp.concatenate(
        [own[:, 0:16], jnp.where(sub < 3, own[:, 16:24], side)], axis=1
    )
    right = jnp.concatenate(
        [own[:, 16:32], jnp.where(sub >= 5, own[:, 8:16], side)], axis=1
    )
    return left, right


def near_masks(first_col):
    qi = iota((QUERIES, KEYS), 0)
    ki = iota((QUERIES, KEYS), 1)
    slot = ki % SLOTS
    row_near = jnp.abs(ki // SLOTS - 3 - qi // HALF) <= 3
    out = []
    for half in range(2):
        if half == 0:
            col = jnp.where(slot < 19, slot, slot - 22)
            real = slot < 22
        else:
            col = jnp.where(slot < 19, slot + 16, slot - 8)
            real = (slot < 19) | (slot >= 21)
        near = jnp.abs(col - (qi % HALF + half * HALF)) <= 3
        place = col + first_col
        inside = (place >= 0) & (place < BREADTH)
        out.append(jnp.where(row_near & near & real & inside, 0.0, NEG))
    return out


def window_block(q, k, v, bias, first):
    tiles = []
    for m in range(2):
        cols = slice(m * 128, (m + 1) * 128)
        queries = pair_queries(q[:, cols], first)
        keys = pair_keys(k[:, cols], first)
        values = pair_values(v[:, cols], first)
        outs = []
        for e in range(2):
            s = scored(queries[e], keys[e]) + bias
            p = jnp.exp(s - jnp.max(s, axis=1, keepdims=True))
            total = jnp.sum(p, axis=1, keepdims=True)
            outs.append(mixed_values(p, values[e]) / total)
        tiles.append(jnp.where(first, outs[0], outs[1]))
    return jnp.concatenate(tiles, axis=1)


def row_bias(first_row):
    row = iota((1, KEYS), 1) // SLOTS - 3 + first_row
    return jnp.where((row >= 0) & (row < HEIGHT), 0.0, NEG)


def places():
    return lax.axis_index(ROW_AXIS) * ROWS, lax.axis_index(COL_AXIS) * COLS


def middle_kernel(
    x_ref, in_ref, out_ref, q_ref, k_ref, v_ref, gain_ref, wp_ref, wo_ref,
    kw_ref, vw_ref, l0_ref, side,
):
    side[...] = jnp.zeros((ROWS, 8, C0), F32)
    left, right = sides(in_ref, out_ref)
    side[:, 0:3, :] = right
    side[:, 3:6, :] = left
    k_side, v_side = keys_values(side[...].reshape(ROWS * 8, C0), gain_ref, wp_ref)
    for ref, own, extra in ((kw_ref, k_ref, k_side), (vw_ref, v_ref, v_side)):
        ref[0], ref[1] = windowed(own[...], extra.reshape(ROWS, 8, C0))
    first_row, first_col = places()
    masks = near_masks(first_col)
    first = iota((1, 128), 1) < HEAD
    for t in (1, 2):
        rows = slice(BLOCK * t, BLOCK * t + BLOCK)
        at = BLOCK * t - 3
        q = q_ref[BLOCK * t * COLS : BLOCK * (t + 1) * COLS, :].reshape(BLOCK, COLS, C0)
        outs = []
        for half in range(2):
            k = kw_ref[half, at : at + WINDOW].reshape(KEYS, C0)
            v = vw_ref[half, at : at + WINDOW].reshape(KEYS, C0)
            now = q[:, half * HALF : (half + 1) * HALF].reshape(QUERIES, C0)
            bias = masks[half] + row_bias(first_row + BLOCK * t)
            outs.append(window_block(now, k, v, bias, first).reshape(BLOCK, HALF, C0))
        attended = jnp.concatenate(outs, axis=1).reshape(BLOCK * COLS, C0)
        l0_ref[BLOCK * COLS * (t - 1) : BLOCK * COLS * t, :] = x_ref[rows].reshape(
            BLOCK * COLS, C0
        ) + mm(attended, wo_ref[...])


def outer_kernel(
    x_ref, in_ref, out_ref, q_ref, kw_ref, vw_ref, mid_ref, gain_ref, wp_ref, wo_ref,
    m1_ref, m2_ref, ggain_ref,
    l0_ref, l1_ref, l2_ref, one_ref, order,
):
    even = lax.axis_index("xl") == 0
    top = jnp.where(even, out_ref[...], in_ref[...])
    bot = jnp.where(even, in_ref[...], out_ref[...])
    raw = jnp.concatenate([top, bot], axis=0).reshape(240, C0)
    k_new, v_new = keys_values(raw, gain_ref, wp_ref)
    k_new = k_new.reshape(6, 40, C0)
    v_new = v_new.reshape(6, 40, C0)
    k_new = windowed(k_new[:, 0:COLS], k_new[:, COLS:])
    v_new = windowed(v_new[:, 0:COLS], v_new[:, COLS:])
    first_row, first_col = places()
    masks = near_masks(first_col)
    first = iota((1, 128), 1) < HEAD
    for t in (0, 3):
        q = q_ref[BLOCK * t * COLS : BLOCK * (t + 1) * COLS, :].reshape(BLOCK, COLS, C0)
        outs = []
        for half in range(2):
            if t == 0:
                k = jnp.concatenate([k_new[half][0:3], kw_ref[half, 0:7]], axis=0)
                v = jnp.concatenate([v_new[half][0:3], vw_ref[half, 0:7]], axis=0)
            else:
                k = jnp.concatenate([kw_ref[half, 9:16], k_new[half][3:6]], axis=0)
                v = jnp.concatenate([vw_ref[half, 9:16], v_new[half][3:6]], axis=0)
            now = q[:, half * HALF : (half + 1) * HALF].reshape(QUERIES, C0)
            bias = masks[half] + row_bias(first_row + BLOCK * t)
            block = window_block(now, k.reshape(KEYS, C0), v.reshape(KEYS, C0), bias, first)
            outs.append(block.reshape(BLOCK, HALF, C0))
        attended = jnp.concatenate(outs, axis=1).reshape(BLOCK * COLS, C0)
        level = x_ref[BLOCK * t : BLOCK * (t + 1)].reshape(BLOCK * COLS, C0) + mm(
            attended, wo_ref[...]
        )
        for half in range(2):
            l0_ref[half, BLOCK * COLS * t : BLOCK * COLS * (t + 1), :] = level[
                :, half * 128 : (half + 1) * 128
            ]
    for half in range(2):
        l0_ref[half, 128:384, :] = mid_ref[:, half * 128 : (half + 1) * 128]
    for n, (a1, b1, a2, b2) in enumerate(CLASSES):
        for i in range(4):
            start = (BLOCK * i + 2 * a2 + a1) * COLS + 2 * b2 + b1
            for half in range(2):
                order[n * 32 + i * 8 : n * 32 + i * 8 + 8, half * 128 : half * 128 + 128] = l0_ref[
                    half, pl.ds(start, 8, stride=4), :
                ]
    one = mm(order[0:128, :], m1_ref[0:C0, :])
    for n in range(1, 4):
        one = one + mm(order[n * 128 : (n + 1) * 128, :], m1_ref[n * C0 : (n + 1) * C0, :])
    l1_ref[...] = one
    two = mm(one[0:32], m2_ref[0:CM, :])
    for n in range(1, 4):
        two = two + mm(one[n * 32 : (n + 1) * 32], m2_ref[n * CM : (n + 1) * CM, :])
    l2_ref[...] = two
    one_ref[...] = rms(two, ggain_ref[...])


def chunks_in(gp_hbm, weight, sems, width):
    copies = []
    for m in range(4):
        cols = slice(384 * m, 384 * m + width)
        copies.append(pltpu.make_async_copy(gp_hbm.at[:, cols], weight.at[:, cols], sems.at[m]))
        copies[-1].start()
    return copies


def query_kernel(x_ref, gp_hbm, scale_hbm, q_ref, weight, scale, sems):
    scale_in = pltpu.make_async_copy(scale_hbm, scale, sems.at[4])
    scale_in.start()
    copies = chunks_in(gp_hbm, weight, sems, 256)
    first = iota((1, 128), 1) < HEAD
    x = x_ref[...]
    scale_in.wait()
    factor = lanes_of(scale, HEADS_G)
    for g in range(2):
        tiles = []
        for m in (2 * g, 2 * g + 1):
            copies[m].wait()
            at = 384 * m
            tiles.append(jnp.where(first, weight[:, at : at + 128], weight[:, at + 128 : at + 256]))
        q = floored(mm(x, jnp.concatenate(tiles, axis=1), HIGHEST))
        q_ref[:, g * 256 : (g + 1) * 256] = q * factor[:, g * 256 : (g + 1) * 256]


def picked(gp_ref, one, other, first):
    tiles = []
    for m in range(4):
        at = 384 * m
        a = gp_ref[:, at + 128 * one : at + 128 * one + 128]
        b = gp_ref[:, at + 128 * other : at + 128 * other + 128]
        tiles.append(jnp.where(first, a, b))
    return jnp.concatenate(tiles, axis=1)


def attention_kernel(x0_ref, x1_ref, x2_ref, x3_ref, q_ref, gp_ref, mine_ref, other_ref, kk, vv):
    first = iota((1, 128), 1) < HEAD
    x = jnp.concatenate([ref[...] for ref in (x0_ref, x1_ref, x2_ref, x3_ref)], axis=0)
    kk[...] = floored(mm(x, picked(gp_ref, 2, 0, first)))
    vv[...] = mm(x, picked(gp_ref, 1, 2, first))
    lane = iota((256, 128), 1)
    extra = jnp.zeros((256, 128), F32)
    q = q_ref[...].reshape(256, CG)
    for m in range(4):
        cols = slice(m * 128, (m + 1) * 128)
        queries = pair_queries(q[:, cols], first)
        keys = pair_keys(kk[:, cols], first)
        values = pair_values(vv[:, cols], first)
        outs = []
        for e in range(2):
            s = scored(queries[e], keys[1 - e])
            best = jnp.max(s, axis=1, keepdims=True)
            p = jnp.exp(s - best)
            outs.append(mixed_values(p, values[e]))
            extra = jnp.where(lane == 2 * m + e, best, extra)
            extra = jnp.where(lane == 8 + 2 * m + e, jnp.sum(p, axis=1, keepdims=True), extra)
        both = jnp.where(first, outs[0], outs[1]).reshape(4, 2, 32, 128)
        mine_ref[:, :, cols] = both[:, 0]
        other_ref[:, :, cols] = both[:, 1]
    both = extra.reshape(4, 2, 32, 128)
    mine_ref[:, :, CG:] = both[:, 0]
    other_ref[:, :, CG:] = both[:, 1]


def spreader():
    return jnp.where(iota((128, CG), 0) == iota((128, CG), 1) // HEAD, 1.0, 0.0)


def merge_kernel(a_ref, b_ref, *out_refs):
    a = a_ref[...].reshape(128, CG + 128)
    b = b_ref[...].reshape(128, CG + 128)
    lane = iota((128, 128), 1)
    best = jnp.maximum(a[:, CG:], b[:, CG:])
    total = jnp.zeros((128, CG), F32)
    sums = jnp.zeros((128, 128), F32)
    for part in (a, b):
        extra = part[:, CG:]
        w = jnp.where(lane < 8, jnp.exp(extra - best), 0.0)
        sums = sums + w * pltpu.roll(extra, 120, 1)
        total = total + mm(w, spreader(), HIGHEST) * part[:, 0:CG]
    extra = jnp.where(lane < 8, best, pltpu.roll(sums, 8, 1))
    for n, ref in enumerate(out_refs):
        ref[:, 0:CG] = total[n * 32 : (n + 1) * 32]
        ref[:, CG:] = extra[n * 32 : (n + 1) * 32]


def tail_kernel(
    p0_ref, p1_ref, p2_ref, p3_ref, l0_ref, l1_ref, l2_ref, go_ref, s2_ref, s1_ref, out_ref, spread
):
    arrived = (p0_ref, p1_ref, p2_ref, p3_ref)
    best = p0_ref[:, CG:]
    for ref in arrived[1:]:
        best = jnp.maximum(best, ref[:, CG:])
    pick = spreader()
    lane = iota((32, 128), 1)
    total = jnp.zeros((32, CG), F32)
    sums = jnp.zeros((32, 128), F32)
    for ref in arrived:
        extra = ref[:, CG:]
        w = jnp.where(lane < 8, jnp.exp(extra - best), 0.0)
        sums = sums + w * pltpu.roll(extra, 120, 1)
        total = total + mm(w, pick, HIGHEST) * ref[:, 0:CG]
    inverse = jnp.where(lane < 8, 1.0 / jnp.where(lane < 8, sums, 1.0), 0.0)
    mixed = l2_ref[...] + mm(total * mm(inverse, pick, HIGHEST), go_ref[...])
    second = mm(mixed, s2_ref[...])
    up = jnp.concatenate(
        [l1_ref[n * 32 : (n + 1) * 32, :] + second[:, n * CM : (n + 1) * CM] for n in range(4)],
        axis=0,
    )
    first = mm(up, s1_ref[...])
    for a1, b1, a2, b2 in CLASSES:
        c1 = a1 * 2 + b1
        c2 = a2 * 2 + b2
        for i in range(4):
            start = (BLOCK * i + 2 * a2 + a1) * COLS + 2 * b2 + b1
            for half in range(2):
                at = c1 * C0 + half * 128
                spread[half, pl.ds(start, 8, stride=4), :] = first[
                    c2 * 32 + i * 8 : c2 * 32 + i * 8 + 8, at : at + 128
                ]
    for half in range(2):
        out_ref[:, :, half * 128 : half * 128 + 128] = (spread[half] + l0_ref[half]).reshape(
            ROWS, COLS, 128
        )


def f32(*shape):
    return jax.ShapeDtypeStruct(shape, F32)


def swaps(value, axis):
    return [lax.ppermute(value, axis, [(i, i ^ d) for i in range(4)]) for d in TURNS]


def odd_swaps(n):
    return [p for i in range(1, n - 1, 2) for p in ((i, i + 1), (i + 1, i))]


V = pl.BlockSpec(memory_space=pltpu.VMEM)
H = pl.BlockSpec(memory_space=pltpu.HBM)
DMA = pltpu.SemaphoreType.DMA


def call(kernel, ins, outs, scratch=(), us=1, megabytes=16):
    many = isinstance(outs, tuple)
    run = pl.pallas_call(
        kernel,
        compiler_params=pltpu.CompilerParams(vmem_limit_bytes=megabytes << 20),
        cost_estimate=pl.CostEstimate(
            flops=int(us * 4e8), transcendentals=0, bytes_accessed=1 << 20
        ),
        out_shape=outs,
        in_specs=[H if i == "h" else V for i in ins],
        out_specs=tuple(V for _ in outs) if many else V,
        scratch_shapes=[pltpu.VMEM(s, F32) if isinstance(s, tuple) else s for s in scratch],
    )

    def placed(*args):
        return run(
            *(
                pltpu.with_memory_space_constraint(a, pltpu.HBM) if i == "h" else a
                for i, a in zip(ins, args)
            )
        )

    return placed


def shards(
    latent, local_gain, local_project, local_output, local_scale, merge_first, merge_second,
    global_gain, global_project, global_output, global_scale, split_second, split_first,
):
    gain = local_gain[None]
    inner, outer = call(edge_kernel, "v", (f32(ROWS, 3, C0), f32(ROWS, 3, C0)))(latent)
    col_in = lax.ppermute(inner, "c", [(0, 1), (1, 0)])
    col_out = lax.ppermute(outer, COL_AXIS, odd_swaps(16))
    q, k, v = call(
        own_kernel,
        "vhhh",
        (f32(512, C0), f32(ROWS, COLS, C0), f32(ROWS, COLS, C0)),
        [(1, C0), (C0, 3 * C0), pltpu.SMEM((HEADS0,), F32), DMA((3,))],
        us=5,
    )(latent, gain, local_project, local_scale)
    inner, outer = call(row_kernel, "vvv", (f32(3, 40, C0), f32(3, 40, C0)))(
        latent, col_in, col_out
    )
    row_in = lax.ppermute(inner, "xl", [(0, 1), (1, 0)])
    row_out = lax.ppermute(outer, ROW_AXIS, odd_swaps(8))
    kw, vw, mid = call(
        middle_kernel,
        "v" * 9,
        (f32(2, ROWS, SLOTS, C0), f32(2, ROWS, SLOTS, C0), f32(256, C0)),
        [(ROWS, 8, C0)],
        us=8,
    )(latent, col_in, col_out, q, k, v, gain, local_project, local_output)
    l0, l1, l2, one = call(
        outer_kernel,
        "v" * 13,
        (f32(2, 512, 128), f32(128, CM), f32(32, CG), f32(32, CG)),
        [(512, C0)],
    )(
        latent, row_in, row_out, q, kw, vw, mid, gain, local_project, local_output,
        merge_first, merge_second, global_gain[None],
    )
    moved = swaps(one, ("xl", "xh"))
    qg = call(
        query_kernel,
        "vhh",
        f32(32, CG),
        [(CG, 3 * CG), pltpu.SMEM((HEADS_G,), F32), DMA((5,))],
        us=4,
    )(one, global_project, global_scale)
    row = jnp.concatenate([one] + moved)
    keys_from = [row] + swaps(row, "z")
    swapped = lax.ppermute(qg, "c", [(0, 1), (1, 0)])
    two = jnp.stack([qg, swapped])
    queries_from = jnp.concatenate([two] + swaps(two, "y"))
    mine, other = call(
        attention_kernel,
        "vvvvvv",
        (f32(4, 32, CG + 128), f32(4, 32, CG + 128)),
        [(512, CG), (512, CG)],
    )(*keys_from, queries_from, global_project)
    theirs = lax.ppermute(other, "c", [(0, 1), (1, 0)])
    merged = call(merge_kernel, "vv", tuple(f32(32, CG + 128) for _ in range(4)))(mine, theirs)
    arrived = [merged[0]] + [
        lax.ppermute(part, "y", [(i, i ^ d) for i in range(4)])
        for part, d in zip(merged[1:], TURNS)
    ]
    return call(tail_kernel, "v" * 10, f32(ROWS, COLS, C0), [(2, 512, 128)])(
        *arrived, l0, l1, l2, global_output, split_second, split_first
    )


def solution(mesh):
    fine = Mesh(mesh.devices.reshape(4, 2, 4, 2, 2), ("z", "xl", "y", "xh", "c"))
    tile = P(ROW_AXIS, COL_AXIS, None)
    return jax.shard_map(
        shards, mesh=fine, in_specs=(tile,) + (P(),) * 12, out_specs=tile, check_vma=False
    )
```
